32 devices in a mesh: py: 2 (over y), px: 4 (over x, core), pz: 4 (over z).
Axes of the slice: x: 2, y: 2, z: 4, core: 2. Of those that a mesh axis runs over, the one named last changes fastest.
Arguments:
- tracer: float32 [32, 512, 32, 128], P('py', 'px', 'pz'), may hold values from 0.2 to 1.8
- conductance: float32 [32, 512, 32, 128], P('py', 'px', 'pz'), may hold values from 0.03 to 0.15
- source: float32 [32, 512, 32, 128], P('py', 'px', 'pz'), may hold values from -0.2 to 0.2
Outputs:
- potential: float32 [32, 512, 32, 128], P('py', 'px', 'pz')
- tracer_end: float32 [32, 512, 32, 128], P('py', 'px', 'pz')
The draws below stay inside these ranges and needn't reach their ends.
All inputs are finite; a program needn't handle non-finite values.
Results may differ from the reference program's by a relative error of at most 0.00002.
Values sent between devices are 32-bit elements; how exact they have to be, the bound alone decides.
No kernel may reach another device: no remote copies, remote signals or barrier semaphores. Data moves between devices by JAX's collectives and lax.ppermute only.
A program may use at most 320 MiB of HBM per device.

```python
import jax
import jax.numpy as jnp
from jax import lax

GRID_Y = 32
GRID_X = 512
GRID_Z = 32
MEMBERS = 128
STEPS = 4


def block_scale(stream_key, shape, shards, least, high):
    factor_of = 1.0
    for position, parts in shards:
        draws = jax.random.uniform(jax.random.fold_in(jax.random.fold_in(stream_key, 6), position), (parts,), jnp.float32, least / len(shards), high / len(shards))
        factor_of = factor_of * jnp.repeat(jnp.exp(draws), shape[position] // parts).reshape((-1,) + (1,) * (len(shape) - 1 - position))
    return factor_of


def setup_inputs(seed: int = 0) -> dict:
    splits = jax.random.split(jax.random.key(seed), 4)
    tracer = jnp.clip(0.2 + 1.5999999 * jax.random.uniform(splits[0], (GRID_Y, GRID_X, GRID_Z, MEMBERS), jnp.float32) ** block_scale(splits[0], (GRID_Y, GRID_X, GRID_Z, MEMBERS), ((0, 2), (1, 4), (2, 4)), -0.2, 0.2), 0.2, 1.8)
    conductance = jnp.clip(0.03 + 0.120000007 * jax.random.uniform(splits[1], (GRID_Y, GRID_X, GRID_Z, MEMBERS), jnp.float32) ** block_scale(splits[1], (GRID_Y, GRID_X, GRID_Z, MEMBERS), ((0, 2), (1, 4), (2, 4)), -0.2, 0.2), 0.03, 0.15)
    source = jnp.clip(jax.random.uniform(splits[2], (GRID_Y, GRID_X, GRID_Z, MEMBERS), jnp.float32, -0.2, 0.2) * block_scale(splits[2], (GRID_Y, GRID_X, GRID_Z, MEMBERS), ((0, 2), (1, 4), (2, 4)), -0.4, 0.0), -0.2, 0.2)
    return dict(tracer=tracer, conductance=conductance, source=source)


def strip_edges(values, dims):
    for dim in dims:
        values = lax.slice_in_dim(values, 1, values.shape[dim] - 1, axis=dim)
    return values


def neighbour(values, dim, start, dims):
    others = [other for other in dims if other != dim]
    values = strip_edges(values, others)
    return lax.slice_in_dim(values, start, start + values.shape[dim] - 2, axis=dim)


def one_step(padded, conductance, source):
    middle = strip_edges(padded, (0, 1, 2))
    lower = [neighbour(padded, dim, 0, (0, 1, 2)) for dim in (0, 1, 2)]
    upper = [neighbour(padded, dim, 2, (0, 1, 2)) for dim in (0, 1, 2)]
    spread = lower[0] + upper[0] + lower[1] + upper[1] + lower[2] + upper[2] - 6.0 * middle
    return middle + conductance * spread + source


def reference(tracer, conductance, source):
    for step in range(STEPS):
        tracer = one_step(jnp.pad(tracer, ((1, 1), (1, 1), (1, 1), (0, 0)), mode="wrap"), conductance, source)
    potential = jnp.cumsum(tracer, axis=2) / GRID_Z
    return potential, tracer
```

```python
import math

import jax
import jax.numpy as jnp
from jax import lax
from jax.experimental import pallas as pl
from jax.experimental.pallas import tpu as pltpu
from jax.sharding import PartitionSpec as P


STEPS = 4
LANES = 8
SHARES = (5, 5, 4, 2)
GROUPS = 4
VMEM_LIMIT = 20 * 1024 * 1024


HBM = pl.BlockSpec(memory_space=pltpu.HBM)
VMEM = pl.BlockSpec(memory_space=pltpu.VMEM)


def pieces_of(width):
    tiles = width // LANES
    total = sum(SHARES)
    ends = [tiles * sum(SHARES[: i + 1]) // total for i in range(len(SHARES))]
    starts = [0] + ends[:-1]
    return [(a * LANES, (b - a) * LANES) for a, b in zip(starts, ends) if b > a]


def groups_of(planes):
    count = math.gcd(planes, GROUPS)
    return count, planes // count


def prepare_kernel(first, width, depth, lead, trail, tracer, *refs):
    refs = refs[len(refs) - (5 + lead + trail) :]
    bottom, top, rows = refs[:3]
    edges = refs[3 : 3 + lead + trail]
    block, sem_in = refs[3 + lead + trail :]
    planes = block.shape[0]
    count, each = groups_of(planes)

    def load(g):
        return pltpu.make_async_copy(
            tracer.at[pl.ds(g * each, each), pl.ds(first * depth, width * depth)],
            block.at[pl.ds(g * each, each)],
            sem_in.at[g],
        )

    for g in range(count):
        load(g).start()
    for g in range(count):
        load(g).wait()
        take_rows(block, bottom, top, g * each, each, width, depth)
    take_sides(block, rows, edges, lead, trail, width, depth)


def take_sides(block, rows, edges, lead, trail, width, depth):
    planes = block.shape[0]
    rows[0] = block[planes - 1]
    rows[1] = block[0]
    columns = ([0] if lead else []) + ([width - 1] if trail else [])
    for column, edge in zip(columns, edges):
        edge[...] = block[:, pl.ds(column * depth, depth), :]


def take_rows(block, low, high, start, planes, width, depth):
    across = width // LANES

    def body(i, carry):
        y = start + i // across
        x = lax.rem(i, across) * LANES
        at = pl.multiple_of(x * depth, LANES * depth)
        low[y, pl.ds(pl.multiple_of(x, LANES), LANES), :] = block[y, pl.ds(at, LANES, stride=depth), :]
        high[y, pl.ds(pl.multiple_of(x, LANES), LANES), :] = block[
            y, pl.ds(at + depth - 1, LANES, stride=depth), :
        ]
        return carry

    lax.fori_loop(0, planes * across, body, 0)


def step_kernel(plan, *refs):
    width, depth, where, first, lead, trail, last, extras = plan
    middle, left, right, lower_y, upper_y, low, high, conductance, source = refs[:9]
    refs = refs[9 + extras :]
    if last:
        field, sums, totals = refs[:3]
        old, coefficient, extra, new, running, sem_in, sem_edge, sem_out = refs[3:]
    else:
        field, bottom, top, rows = refs[:4]
        edges = refs[4 : 4 + lead + trail]
        old, coefficient, extra, new, sem_in, sem_edge, sem_out = refs[4 + lead + trail :]
    planes = new.shape[0]
    count, each = groups_of(planes)
    cells = width * depth
    across = width // LANES

    def load(kind, g):
        span = pl.ds(g * each, each)
        if kind == 0:
            return pltpu.make_async_copy(
                middle.at[span, pl.ds(where[0] * depth, cells)],
                old.at[pl.ds(g * each + 1, each), pl.ds(depth, cells)],
                sem_in.at[0, g],
            )
        from_ref, to_ref = ((conductance, coefficient), (source, extra))[kind - 1]
        return pltpu.make_async_copy(
            from_ref.at[span, pl.ds(first * depth, cells)], to_ref.at[span], sem_in.at[kind, g]
        )

    side_loads = []
    for n, (side, is_outer, column) in enumerate(((left, lead, 0), (right, trail, cells + depth))):
        if not is_outer:
            side_loads.append(
                pltpu.make_async_copy(
                    side.at[:, pl.ds(where[1 + n] * depth, depth)],
                    old.at[pl.ds(1, planes), pl.ds(column, depth)],
                    sem_edge.at[n],
                )
            )
    for copy in side_loads:
        copy.start()
    for g in range(count):
        for kind in range(3):
            load(kind, g).start()
    for side, is_outer, column in ((left, lead, 0), (right, trail, cells + depth)):
        if is_outer:
            old[pl.ds(1, planes), pl.ds(column, depth), :] = side[...]
    old[0, pl.ds(depth, cells), :] = lower_y[where[3]]
    old[planes + 1, pl.ds(depth, cells), :] = upper_y[where[4]]
    for copy in side_loads:
        copy.wait()
    load(0, 0).wait()

    here = lax.broadcasted_iota(jnp.int32, (depth, new.shape[2]), 0)
    at_low = here == 0
    at_high = here == depth - 1

    def column_block(i, start):
        y = start + i // across
        x = pl.multiple_of(lax.rem(i, across) * LANES, LANES)
        at = pl.multiple_of(x * depth, LANES * depth)
        before = old[y + 1, pl.ds(at, depth), :]
        centre = old[y + 1, pl.ds(at + depth, depth), :]
        for j in range(LANES):
            row = at + j * depth
            after = old[y + 1, pl.ds(row + 2 * depth, depth), :]
            below = low[y, pl.ds(x + j, depth, stride=0), :]
            above = high[y, pl.ds(x + j, depth, stride=0), :]
            below = jnp.where(at_low, below, pltpu.roll(centre, 1, 0))
            above = jnp.where(at_high, above, pltpu.roll(centre, depth - 1, 0))
            near = old[y, pl.ds(row + depth, depth), :] + old[y + 2, pl.ds(row + depth, depth), :]
            near = near + (before + after) + (below + above) - 6.0 * centre
            new[y, pl.ds(row, depth), :] = (
                centre + coefficient[y, pl.ds(row, depth), :] * near + extra[y, pl.ds(row, depth), :]
            )
            before, centre = centre, after

    def sum_block(i, start):
        y = start + i // across
        x = pl.multiple_of(lax.rem(i, across) * LANES, LANES)
        at = pl.multiple_of(x * depth, LANES * depth)
        so_far = new[y, pl.ds(at, LANES, stride=depth), :]
        running[y, pl.ds(at, LANES, stride=depth), :] = so_far
        for z in range(1, depth):
            so_far = so_far + new[y, pl.ds(at + z, LANES, stride=depth), :]
            running[y, pl.ds(at + z, LANES, stride=depth), :] = so_far
        totals[y, pl.ds(x, LANES), :] = so_far

    def save(g):
        span = pl.ds(g * each, each)
        target = field.at[span, pl.ds(first * depth, cells)] if last else field.at[span]
        return pltpu.make_async_copy(new.at[span], target, sem_out.at[0, g])

    def save_sums(g):
        span = pl.ds(g * each, each)
        return pltpu.make_async_copy(running.at[span], sums.at[span], sem_out.at[1, g])

    for g in range(count):
        if g + 1 < count:
            load(0, g + 1).wait()
        load(1, g).wait()
        load(2, g).wait()

        def walk(i, carry):
            column_block(i, g * each)
            return carry

        lax.fori_loop(0, each * across, walk, 0)
        save(g).start()
        if last:

            def walk_sums(i, carry):
                sum_block(i, g * each)
                return carry

            lax.fori_loop(0, each * across, walk_sums, 0)
            save_sums(g).start()
        else:
            take_rows(new, bottom, top, g * each, each, width, depth)
    if not last:
        take_sides(new, rows, edges, lead, trail, width, depth)
    for g in range(count):
        save(g).wait()
        if last:
            save_sums(g).wait()


def potential_kernel(plan, *refs):
    width, depth, first, earlier, scale, extras = plan
    sums = refs[0]
    offsets = refs[1 : 1 + earlier]
    potential, here, out, sem_in, sem_out = refs[1 + earlier + extras :]
    planes = here.shape[0]
    count, each = groups_of(planes)
    cells = width * depth
    across = width // LANES

    def load(g):
        span = pl.ds(g * each, each)
        return pltpu.make_async_copy(sums.at[span], here.at[span], sem_in.at[g])

    def save(g):
        span = pl.ds(g * each, each)
        return pltpu.make_async_copy(
            out.at[span], potential.at[span, pl.ds(first * depth, cells)], sem_out.at[g]
        )

    for g in range(count):
        load(g).start()
    for g in range(count):
        load(g).wait()

        def walk(i, carry):
            y = g * each + i // across
            x = pl.multiple_of(lax.rem(i, across) * LANES, LANES)
            for j in range(LANES):
                total = offsets[0][y, pl.ds(x + j, depth, stride=0), :]
                for offset in offsets[1:]:
                    total = total + offset[y, pl.ds(x + j, depth, stride=0), :]
                span = pl.ds(pl.multiple_of(x * depth + j * depth, depth), depth)
                value = here[y, span, :] + total
                out[y, span, :] = value * scale[0] if scale[1] else value / scale[0]
            return carry

        lax.fori_loop(0, each * across, walk, 0)
        save(g).start()
    for g in range(count):
        save(g).wait()


def ring(axis):
    count = lax.axis_size(axis)
    forward = [(i, (i + 1) % count) for i in range(count)]
    return forward, [(target, origin) for origin, target in forward]


def on_device(tracer, conductance, source):
    shape = tracer.shape
    planes, columns, depth, members = shape
    pieces = pieces_of(columns)
    last_piece = len(pieces) - 1
    flat = (planes, columns * depth, members)
    tracer, conductance, source = (v.reshape(flat) for v in (tracer, conductance, source))
    count, _ = groups_of(planes)

    def array(*dims):
        return pltpu.HBM(dims, jnp.float32)

    def near(*dims):
        return pltpu.VMEM(dims, jnp.float32)

    def placed(arrays, specs):
        return [
            pltpu.with_memory_space_constraint(v, pltpu.VMEM if spec is VMEM else pltpu.HBM)
            for v, spec in zip(arrays, specs)
        ]

    def scratch(*dims):
        return pltpu.VMEM(dims, jnp.float32)

    def ends(k):
        return int(k == 0), int(k == last_piece)

    def outer_arrays(k):
        width = pieces[k][1]
        lead, trail = ends(k)
        return [
            near(planes, width, members),
            near(planes, width, members),
            near(2, width * depth, members),
        ] + [near(planes, depth, members)] * (lead + trail)

    def prepare(k, token):
        first, width = pieces[k]
        lead, trail = ends(k)

        def kernel(*refs):
            prepare_kernel(first, width, depth, lead, trail, *refs)

        outs = outer_arrays(k)
        return pl.pallas_call(
            kernel,
            out_shape=outs,
            in_specs=[HBM] + [VMEM] * len(token),
            out_specs=[VMEM] * len(outs),
            scratch_shapes=[
                scratch(planes, width * depth, members),
                pltpu.SemaphoreType.DMA((count,)),
            ],
            compiler_params=pltpu.CompilerParams(vmem_limit_bytes=VMEM_LIMIT),
        )(*placed([tracer] + token, [HBM] + [VMEM] * len(token)))

    def advance(k, last, where, operands, whole, token):
        first, width = pieces[k]
        lead, trail = ends(k)
        specs = [HBM, VMEM if lead else HBM, VMEM if trail else HBM] + [VMEM] * 4 + [HBM] * 2
        aliases = {}
        operands = operands + token
        specs = specs + [HBM] * len(token)
        if last and k > 0:
            aliases = {len(operands): 0}
            operands = operands + [whole]
            specs = specs + [HBM]
        plan = (width, depth, where, first, lead, trail, last, len(operands) - 9)

        def kernel(*refs):
            step_kernel(plan, *refs)

        cells = width * depth
        if last:
            outs = [array(*flat), array(planes, cells, members), near(planes, width, members)]
            out_specs = [HBM, HBM, VMEM]
        else:
            outs = [array(planes, cells, members)] + outer_arrays(k)
            out_specs = [HBM] + [VMEM] * (len(outs) - 1)
        return pl.pallas_call(
            kernel,
            out_shape=outs,
            in_specs=specs,
            out_specs=out_specs,
            input_output_aliases=aliases,
            scratch_shapes=[
                scratch(planes + 2, cells + 2 * depth, members),
                scratch(planes, cells, members),
                scratch(planes, cells, members),
                scratch(planes, cells, members),
            ]
            + [scratch(planes, cells, members)] * last
            + [
                pltpu.SemaphoreType.DMA((3, count)),
                pltpu.SemaphoreType.DMA((2,)),
                pltpu.SemaphoreType.DMA((2, count)),
            ],
            compiler_params=pltpu.CompilerParams(vmem_limit_bytes=VMEM_LIMIT),
        )(*placed(operands, specs))

    def finish(k, sums, offsets, whole, scale):
        first, width = pieces[k]
        cells = width * depth
        operands = [sums] + offsets
        specs = [HBM] + [VMEM] * len(offsets)
        aliases = {}
        if k > 0:
            aliases = {len(operands): 0}
            operands = operands + [whole]
            specs = specs + [HBM]
        plan = (width, depth, first, len(offsets), scale, len(operands) - 1 - len(offsets))

        def kernel(*refs):
            potential_kernel(plan, *refs)

        return pl.pallas_call(
            kernel,
            out_shape=[array(*flat)],
            in_specs=specs,
            out_specs=[HBM],
            input_output_aliases=aliases,
            scratch_shapes=[
                scratch(planes, cells, members),
                scratch(planes, cells, members),
                pltpu.SemaphoreType.DMA((count,)),
                pltpu.SemaphoreType.DMA((count,)),
            ],
            compiler_params=pltpu.CompilerParams(vmem_limit_bytes=VMEM_LIMIT),
        )(*placed(operands, specs))[0]

    z_up, z_down = ring("pz")
    y_up, y_down = ring("py")
    x_up, x_down = ring("px")

    def exchange(k, outer, sides):
        bottom, top, rows = outer[:3]
        edges = list(outer[3:])
        from_below = lax.ppermute(top, "pz", z_up)
        from_above = lax.ppermute(bottom, "pz", z_down)
        if len(y_up) <= 2:
            rows = lax.ppermute(rows, "py", y_up)
            lower_y, upper_y = (rows, 0), (rows, 1)
        else:
            lower_y = (lax.ppermute(rows[0:1], "py", y_up), 0)
            upper_y = (lax.ppermute(rows[1:2], "py", y_down), 0)
        lead, trail = ends(k)
        if lead:
            sides["right"] = lax.ppermute(edges.pop(0), "px", x_down)
        if trail:
            sides["left"] = lax.ppermute(edges.pop(0), "px", x_up)
        return lower_y, upper_y, from_below, from_above

    halos, sides, token = [], {}, []
    for k in range(len(pieces)):
        outer = prepare(k, token)
        token = [outer[0]]
        halos.append(exchange(k, outer, sides))
    token = []
    fields = None
    end, sums, totals = None, [], []
    for step in range(STEPS):
        last = step == STEPS - 1
        next_fields, next_halos, next_sides = [], [], {}
        for k, (first, width) in enumerate(pieces):
            lower_y, upper_y, from_below, from_above = halos[k]
            if step == 0:
                middle = (tracer, first)
                left = (tracer, first - 1)
                right = (tracer, first + width)
            else:
                middle = (fields[k], 0)
                left = (fields[k - 1], pieces[k - 1][1] - 1) if k > 0 else None
                right = (fields[k + 1], 0) if k < last_piece else None
            if k == 0:
                left = (sides["left"], 0)
            if k == last_piece:
                right = (sides["right"], 0)
            where = (middle[1], left[1], right[1], lower_y[1], upper_y[1])
            operands = [
                middle[0], left[0], right[0], lower_y[0], upper_y[0],
                from_below, from_above, conductance, source,
            ]
            results = advance(k, last, where, operands, end, token)
            token = [results[0]] if not last else []
            if last:
                end = results[0]
                sums.append(results[1])
                totals.append(results[2])
            else:
                next_fields.append(results[0])
                next_halos.append(exchange(k, results[1:], next_sides))
        fields, halos, sides = next_fields, next_halos, next_sides

    blocks = lax.axis_size("pz")
    cells_along = depth * blocks
    exact = cells_along & (cells_along - 1) == 0
    scale = (1.0 / cells_along, True) if exact else (float(cells_along), False)
    potential = None
    for k in range(len(pieces)):
        carried, offsets = totals[k], []
        for hop in range(blocks - 1):
            arrived = lax.ppermute(carried, "pz", [(hop, hop + 1)])
            offsets.append(arrived)
            carried = carried + arrived
        potential = finish(k, sums[k], offsets, potential, scale)
    return (potential.reshape(shape), end.reshape(shape))


def solution(mesh):
    placed = P("py", "px", "pz", None)

    return jax.shard_map(
        on_device,
        mesh=mesh,
        in_specs=(placed, placed, placed),
        out_specs=(placed, placed),
        check_vma=False,
    )
```

```python
import math

import jax
import jax.numpy as jnp
from jax import lax
from jax.experimental import pallas as pl
from jax.experimental.pallas import tpu as pltpu
from jax.sharding import PartitionSpec as P


STEPS = 4
ROWS = 8
SHARES = (5, 5, 4, 2)
GROUPS = 4
LONGEST = 5
VMEM_LIMIT = 10 * 1024 * 1024


HBM = pl.BlockSpec(memory_space=pltpu.HBM)
VMEM = pl.BlockSpec(memory_space=pltpu.VMEM)


def pieces_of(width):
    tiles = width // ROWS
    total = sum(SHARES)
    ends = [tiles * sum(SHARES[: i + 1]) // total for i in range(len(SHARES))]
    starts = [0] + ends[:-1]
    return [(a * ROWS, (b - a) * ROWS) for a, b in zip(starts, ends)]


def groups_of(planes):
    count = math.gcd(planes, GROUPS)
    return count, planes // count


def spans_of(planes, count):
    ends = [planes * (n + 1) // count for n in range(count)]
    return [(a, b - a) for a, b in zip([0] + ends[:-1], ends)]


def parts_of(k):
    return max(1, math.ceil(SHARES[k] / LONGEST))


def take_rows(block, bottom, top, y, width, depth):
    for x in range(0, width, ROWS):
        bottom[y, pl.ds(x, ROWS), :] = block[y, pl.ds(x * depth, ROWS, stride=depth), :]
        top[y, pl.ds(x, ROWS), :] = block[y, pl.ds(x * depth + depth - 1, ROWS, stride=depth), :]


def take_sides(block, rows, edges, lead, trail, width, depth):
    planes = block.shape[0]
    rows[0] = block[planes - 1]
    rows[1] = block[0]
    columns = ([0] if lead else []) + ([width - 1] if trail else [])
    for column, edge in zip(columns, edges):
        edge[...] = block[:, pl.ds(column * depth, depth), :]


def prepare_kernel(plan, tracer, *refs):
    first, width, depth, lead, trail, extras = plan
    refs = refs[extras:]
    block, bottom, top, rows = refs[:4]
    edges = refs[4 : 4 + lead + trail]
    (sem_in,) = refs[4 + lead + trail :]
    planes = block.shape[0]
    count, each = groups_of(planes)

    def load(g):
        span = pl.ds(g * each, each)
        return pltpu.make_async_copy(
            tracer.at[span, pl.ds(first * depth, width * depth)], block.at[span], sem_in.at[g]
        )

    for g in range(count):
        load(g).start()
    for g in range(count):
        load(g).wait()
        for y in range(g * each, (g + 1) * each):
            take_rows(block, bottom, top, y, width, depth)
    take_sides(block, rows, edges, lead, trail, width, depth)


def scaled(value, scale):
    return value * scale[0] if scale[1] else value / scale[0]


def step_kernel(plan, *refs):
    width, depth, first, where, lead, trail, load_rest, last, parts, scale, extras = plan
    old, left, right, lower_y, upper_y, low, high, conductance, source = refs[:9]
    refs = refs[9 + extras :]
    if last:
        field, sums = refs[:2]
        totals = refs[2 : 2 + parts]
        new = refs[2 + parts]
        refs = refs[3 + parts :]
    else:
        new, bottom, top, rows = refs[:4]
        edges = refs[4 : 4 + lead + trail]
        refs = refs[4 + lead + trail :]
    planes = new.shape[0]
    cells = width * depth
    spans = spans_of(planes, parts if last else math.gcd(planes, GROUPS) if load_rest else 1)
    loads = []
    if load_rest:
        coefficient, extra, sem_in = refs[0], refs[1], refs[2]
        refs = refs[3:]
        for g, span in enumerate(spans):
            span = pl.ds(*span)
            part = pl.ds(first * depth, cells)
            loads.append(
                [
                    pltpu.make_async_copy(ref.at[span, part], to.at[span], sem_in.at[n, g])
                    for n, (ref, to) in enumerate(((conductance, coefficient), (source, extra)))
                ]
            )
            for copy in loads[-1]:
                copy.start()
    else:
        coefficient, extra = conductance, source

    here = lax.broadcasted_iota(jnp.int32, (depth, new.shape[2]), 0)
    at_low = here == 0
    at_high = here == depth - 1

    def plane(y, before_y, after_y, g):
        def column(x):
            if x < 0:
                return left[y, pl.ds(where[0] * depth, depth), :]
            if x == width:
                return right[y, pl.ds(where[1] * depth, depth), :]
            return old[y, pl.ds(x * depth, depth), :]

        before, centre = column(-1), column(0)
        for x in range(width):
            span = pl.ds(x * depth, depth)
            after = column(x + 1)
            below = jnp.where(at_low, low[y, pl.ds(x, depth, stride=0), :], pltpu.roll(centre, 1, 0))
            above = jnp.where(
                at_high, high[y, pl.ds(x, depth, stride=0), :], pltpu.roll(centre, depth - 1, 0)
            )
            near = (before_y(span) + after_y(span)) + (before + after) + (below + above) - 6.0 * centre
            new[y, span, :] = centre + coefficient[y, span, :] * near + extra[y, span, :]
            before, centre = centre, after
        if last:
            for x in range(0, width, ROWS):
                total = None
                for z in range(depth):
                    span = pl.ds(x * depth + z, ROWS, stride=depth)
                    value = scaled(new[y, span, :], scale)
                    total = value if z == 0 else total + value
                    sums[y, span, :] = total
                totals[g][y - spans[g][0], pl.ds(x, ROWS), :] = total
        else:
            take_rows(new, bottom, top, y, width, depth)

    def of_plane(y):
        return lambda span: old[y, span, :]

    def outer(ref, row):
        return lambda span: ref[row, span, :]

    def save(g):
        span = pl.ds(*spans[g])
        return pltpu.make_async_copy(
            new.at[span], field.at[span, pl.ds(first * depth, cells)], refs[0].at[g]
        )

    for g, (start, length) in enumerate(spans):
        for copy in loads[g] if load_rest else []:
            copy.wait()
        stop = start + length
        if start == 0:
            plane(0, outer(lower_y, where[2]), of_plane(1), g)
            start = 1
        top_plane = stop == planes
        if top_plane:
            stop = planes - 1

        def walk(y, carry):
            plane(y, of_plane(y - 1), of_plane(y + 1), g)
            return carry

        lax.fori_loop(start, stop, walk, 0)
        if top_plane:
            plane(planes - 1, of_plane(planes - 2), outer(upper_y, where[3]), g)
        if last:
            save(g).start()
    if last:
        for g in range(len(spans)):
            save(g).wait()
    else:
        take_sides(new, rows, edges, lead, trail, width, depth)


def potential_kernel(plan, *refs):
    width, depth, first, parts, earlier, extras = plan
    sums = refs[0]
    offsets = refs[1 : 1 + parts * earlier]
    potential, out, sem_out = refs[1 + parts * earlier + extras :]
    spans = spans_of(sums.shape[0], parts)

    def save(g):
        span = pl.ds(*spans[g])
        return pltpu.make_async_copy(
            out.at[span], potential.at[span, pl.ds(first * depth, width * depth)], sem_out.at[g]
        )

    for g, (start, length) in enumerate(spans):
        below = offsets[g * earlier : (g + 1) * earlier]

        def walk(y, carry):
            for x in range(width):
                row = pl.ds(x, depth, stride=0)
                total = below[0][y - start, row, :]
                for offset in below[1:]:
                    total = total + offset[y - start, row, :]
                span = pl.ds(x * depth, depth)
                out[y, span, :] = sums[y, span, :] + total
            return carry

        lax.fori_loop(start, start + length, walk, 0)
        save(g).start()
    for g in range(parts):
        save(g).wait()


def ring(axis):
    count = lax.axis_size(axis)
    forward = [(i, (i + 1) % count) for i in range(count)]
    return forward, [(target, origin) for origin, target in forward]


def on_device(tracer, conductance, source):
    shape = tracer.shape
    planes, columns, depth, members = shape
    pieces = pieces_of(columns)
    last_piece = len(pieces) - 1
    flat = (planes, columns * depth, members)
    tracer, conductance, source = (v.reshape(flat) for v in (tracer, conductance, source))
    count, _ = groups_of(planes)

    def far(*dims):
        return pltpu.HBM(dims, jnp.float32)

    def near(*dims):
        return pltpu.VMEM(dims, jnp.float32)

    def call(kernel, operands, specs, outs, out_specs, scratch=(), aliases=None):
        operands = [
            pltpu.with_memory_space_constraint(v, pltpu.VMEM if spec is VMEM else pltpu.HBM)
            for v, spec in zip(operands, specs)
        ]
        return pl.pallas_call(
            kernel,
            out_shape=outs,
            in_specs=specs,
            out_specs=out_specs,
            input_output_aliases=aliases or {},
            scratch_shapes=list(scratch),
            compiler_params=pltpu.CompilerParams(vmem_limit_bytes=VMEM_LIMIT),
        )(*operands)

    def ends(k):
        return int(k == 0), int(k == last_piece)

    def block(k):
        return near(planes, pieces[k][1] * depth, members)

    def outer_arrays(k):
        width = pieces[k][1]
        return [
            near(planes, width, members),
            near(planes, width, members),
            near(2, width * depth, members),
        ] + [near(planes, depth, members)] * sum(ends(k))

    def prepare(k, token):
        plan = (*pieces[k], depth, *ends(k), len(token))

        def kernel(*refs):
            prepare_kernel(plan, *refs)

        outs = [block(k)] + outer_arrays(k)
        return call(
            kernel,
            [tracer] + token,
            [HBM] + [VMEM] * len(token),
            outs,
            [VMEM] * len(outs),
            [pltpu.SemaphoreType.DMA((count,))],
        )

    def advance(k, step, where, operands, whole, token):
        first, width = pieces[k]
        load_rest, last = step == 0, step == STEPS - 1
        rest = HBM if load_rest else VMEM
        specs = [VMEM] * 7 + [rest] * 2 + [VMEM] * len(token)
        operands = operands + token
        aliases = {}
        if last and k > 0:
            aliases = {len(operands): 0}
            operands = operands + [whole]
            specs = specs + [HBM]
        parts = parts_of(k)
        plan = (width, depth, first, where, *ends(k), load_rest, last, parts, scale, len(operands) - 9)

        def kernel(*refs):
            step_kernel(plan, *refs)

        if last:
            outs = [far(*flat), block(k)]
            outs += [near(length, width, members) for _, length in spans_of(planes, parts)]
            out_specs = [HBM] + [VMEM] * (1 + parts)
            scratch = [
                pltpu.VMEM((planes, width * depth, members), jnp.float32),
                pltpu.SemaphoreType.DMA((parts,)),
            ]
        else:
            outs = [block(k)] + outer_arrays(k) + [block(k)] * (2 * load_rest)
            out_specs = [VMEM] * len(outs)
            scratch = [pltpu.SemaphoreType.DMA((2, count))] * load_rest
        return call(kernel, operands, specs, outs, out_specs, scratch, aliases)

    def finish(k, sums, offsets, whole):
        first, width = pieces[k]
        parts, earlier = len(offsets), len(offsets[0])
        operands = [sums] + [v for part in offsets for v in part]
        specs = [VMEM] * len(operands)
        aliases = {}
        if k > 0:
            aliases = {len(operands): 0}
            operands = operands + [whole]
            specs = specs + [HBM]
        extras = len(operands) - 1 - parts * earlier
        plan = (width, depth, first, parts, earlier, extras)

        def kernel(*refs):
            potential_kernel(plan, *refs)

        scratch = [
            pltpu.VMEM((planes, width * depth, members), jnp.float32),
            pltpu.SemaphoreType.DMA((parts,)),
        ]
        return call(kernel, operands, specs, [far(*flat)], [HBM], scratch, aliases)[0]

    blocks = lax.axis_size("pz")
    cells_along = depth * blocks
    exact = cells_along & (cells_along - 1) == 0
    scale = (1.0 / cells_along, True) if exact else (float(cells_along), False)
    z_up, z_down = ring("pz")
    y_up, y_down = ring("py")
    x_up, x_down = ring("px")

    def exchange(k, outer, sides):
        bottom, top, rows = outer[:3]
        edges = list(outer[3:])
        from_below = lax.ppermute(top, "pz", z_up)
        from_above = lax.ppermute(bottom, "pz", z_down)
        if len(y_up) <= 2:
            rows = lax.ppermute(rows, "py", y_up)
            lower_y, upper_y = (rows, 0), (rows, 1)
        else:
            lower_y = (lax.ppermute(rows[0:1], "py", y_up), 0)
            upper_y = (lax.ppermute(rows[1:2], "py", y_down), 0)
        lead, trail = ends(k)
        if lead:
            sides["right"] = lax.ppermute(edges.pop(0), "px", x_down)
        if trail:
            sides["left"] = lax.ppermute(edges.pop(0), "px", x_up)
        return lower_y, upper_y, from_below, from_above

    fields, rest, halos, sides, token = [], [], [], {}, []
    for k in range(len(pieces)):
        field, *outer = prepare(k, token)
        token = [outer[0]]
        fields.append(field)
        rest.append((conductance, source))
        halos.append(exchange(k, outer, sides))
    token = []
    end, totals = None, []
    for step in range(STEPS):
        next_fields, next_halos, next_sides = [], [], {}
        for k, (first, width) in enumerate(pieces):
            lower_y, upper_y, from_below, from_above = halos[k]
            left = (fields[k - 1], pieces[k - 1][1] - 1) if k > 0 else (sides["left"], 0)
            right = (fields[k + 1], 0) if k < last_piece else (sides["right"], 0)
            where = (left[1], right[1], lower_y[1], upper_y[1])
            operands = [fields[k], left[0], right[0], lower_y[0], upper_y[0]]
            operands += [from_below, from_above, *rest[k]]
            results = list(advance(k, step, where, operands, end, token))
            if step == STEPS - 1:
                end, field, *total = results
                token = []
                next_fields.append(field)
                totals.append(total)
                continue
            if step == 0:
                rest[k] = tuple(results[-2:])
                results = results[:-2]
            token = [results[1]]
            next_fields.append(results[0])
            next_halos.append(exchange(k, results[1:], next_sides))
        fields, halos, sides = next_fields, next_halos, next_sides

    potential = None
    for k in range(len(pieces)):
        offsets = []
        for carried in totals[k]:
            offsets.append([])
            for hop in range(blocks - 1):
                arrived = lax.ppermute(carried, "pz", [(hop, hop + 1)])
                offsets[-1].append(arrived)
                carried = carried + arrived
        potential = finish(k, fields[k], offsets, potential)
    return (potential.reshape(shape), end.reshape(shape))


def solution(mesh):
    placed = P("py", "px", "pz", None)

    return jax.shard_map(
        on_device,
        mesh=mesh,
        in_specs=(placed, placed, placed),
        out_specs=(placed, placed),
        check_vma=False,
    )
```

```python
import math

import jax
import jax.numpy as jnp
from jax import lax
from jax.experimental import pallas as pl
from jax.experimental.pallas import tpu as pltpu
from jax.sharding import PartitionSpec as P


STEPS = 4
ROWS = 8
SHARES = (5, 4, 4, 3)
GROUPS = 4
PARTS = (1, 1, 1, 2)
VMEM_LIMIT = 10 * 1024 * 1024


HBM = pl.BlockSpec(memory_space=pltpu.HBM)
VMEM = pl.BlockSpec(memory_space=pltpu.VMEM)


def pieces_of(width):
    tiles = width // ROWS
    total = sum(SHARES)
    ends = [tiles * sum(SHARES[: i + 1]) // total for i in range(len(SHARES))]
    starts = [0] + ends[:-1]
    return [(a * ROWS, (b - a) * ROWS) for a, b in zip(starts, ends)]


def groups_of(planes):
    count = math.gcd(planes, GROUPS)
    return count, planes // count


def spans_of(planes, count):
    ends = [planes * (n + 1) // count for n in range(count)]
    return [(a, b - a) for a, b in zip([0] + ends[:-1], ends)]


def parts_of(k):
    return PARTS[k]


def take_rows(block, bottom, top, y, width, depth):
    for x in range(0, width, ROWS):
        bottom[y, pl.ds(x, ROWS), :] = block[y, pl.ds(x * depth, ROWS, stride=depth), :]
        top[y, pl.ds(x, ROWS), :] = block[y, pl.ds(x * depth + depth - 1, ROWS, stride=depth), :]


def take_sides(block, rows, edges, lead, trail, width, depth):
    planes = block.shape[0]
    rows[0] = block[planes - 1]
    rows[1] = block[0]
    columns = ([0] if lead else []) + ([width - 1] if trail else [])
    for column, edge in zip(columns, edges):
        edge[...] = block[:, pl.ds(column * depth, depth), :]


def prepare_kernel(plan, tracer, *refs):
    first, width, depth, lead, trail, extras = plan
    refs = refs[extras:]
    block, bottom, top, rows = refs[:4]
    edges = refs[4 : 4 + lead + trail]
    (sem_in,) = refs[4 + lead + trail :]
    planes = block.shape[0]
    count, each = groups_of(planes)

    def load(g):
        span = pl.ds(g * each, each)
        return pltpu.make_async_copy(
            tracer.at[span, pl.ds(first * depth, width * depth)], block.at[span], sem_in.at[g]
        )

    for g in range(count):
        load(g).start()
    for g in range(count):
        load(g).wait()
        for y in range(g * each, (g + 1) * each):
            take_rows(block, bottom, top, y, width, depth)
    take_sides(block, rows, edges, lead, trail, width, depth)


def scaled(value, scale):
    return value * scale[0] if scale[1] else value / scale[0]


def step_kernel(plan, *refs):
    width, depth, first, where, lead, trail, load_rest, last, parts, scale, extras = plan
    old, left, right, lower_y, upper_y, low, high, conductance, source = refs[:9]
    refs = refs[9 + extras :]
    if last:
        field, sums = refs[:2]
        totals = refs[2 : 2 + parts]
        new = refs[2 + parts]
        refs = refs[3 + parts :]
    else:
        new, bottom, top, rows = refs[:4]
        edges = refs[4 : 4 + lead + trail]
        refs = refs[4 + lead + trail :]
    planes = new.shape[0]
    cells = width * depth
    spans = spans_of(planes, parts if last else math.gcd(planes, GROUPS) if load_rest else 1)
    loads = []
    if load_rest:
        coefficient, extra, sem_in = refs[0], refs[1], refs[2]
        refs = refs[3:]
        for g, span in enumerate(spans):
            span = pl.ds(*span)
            part = pl.ds(first * depth, cells)
            loads.append(
                [
                    pltpu.make_async_copy(ref.at[span, part], to.at[span], sem_in.at[n, g])
                    for n, (ref, to) in enumerate(((conductance, coefficient), (source, extra)))
                ]
            )
            for copy in loads[-1]:
                copy.start()
    else:
        coefficient, extra = conductance, source

    here = lax.broadcasted_iota(jnp.int32, (depth, new.shape[2]), 0)
    at_low = here == 0
    at_high = here == depth - 1

    def plane(y, before_y, after_y, g):
        def column(x):
            if x < 0:
                return left[y, pl.ds(where[0] * depth, depth), :]
            if x == width:
                return right[y, pl.ds(where[1] * depth, depth), :]
            return old[y, pl.ds(x * depth, depth), :]

        before, centre = column(-1), column(0)
        for x in range(width):
            span = pl.ds(x * depth, depth)
            after = column(x + 1)
            below = jnp.where(at_low, low[y, pl.ds(x, depth, stride=0), :], pltpu.roll(centre, 1, 0))
            above = jnp.where(
                at_high, high[y, pl.ds(x, depth, stride=0), :], pltpu.roll(centre, depth - 1, 0)
            )
            near = (before_y(span) + after_y(span)) + (before + after) + (below + above) - 6.0 * centre
            new[y, span, :] = centre + coefficient[y, span, :] * near + extra[y, span, :]
            before, centre = centre, after
        if last:
            for x in range(0, width, ROWS):
                total = None
                for z in range(depth):
                    span = pl.ds(x * depth + z, ROWS, stride=depth)
                    value = scaled(new[y, span, :], scale)
                    total = value if z == 0 else total + value
                    sums[y, span, :] = total
                totals[g][y - spans[g][0], pl.ds(x, ROWS), :] = total
        else:
            take_rows(new, bottom, top, y, width, depth)

    def of_plane(y):
        return lambda span: old[y, span, :]

    def outer(ref, row):
        return lambda span: ref[row, span, :]

    def save(g):
        span = pl.ds(*spans[g])
        return pltpu.make_async_copy(
            new.at[span], field.at[span, pl.ds(first * depth, cells)], refs[0].at[g]
        )

    for g, (start, length) in enumerate(spans):
        for copy in loads[g] if load_rest else []:
            copy.wait()
        stop = start + length
        if start == 0:
            plane(0, outer(lower_y, where[2]), of_plane(1), g)
            start = 1
        top_plane = stop == planes
        if top_plane:
            stop = planes - 1

        def walk(y, carry):
            plane(y, of_plane(y - 1), of_plane(y + 1), g)
            return carry

        lax.fori_loop(start, stop, walk, 0)
        if top_plane:
            plane(planes - 1, of_plane(planes - 2), outer(upper_y, where[3]), g)
        if last:
            save(g).start()
    if last:
        for g in range(len(spans)):
            save(g).wait()
    else:
        take_sides(new, rows, edges, lead, trail, width, depth)


def potential_kernel(plan, *refs):
    width, depth, first, parts, earlier, extras = plan
    sums = refs[0]
    offsets = refs[1 : 1 + parts * earlier]
    potential, out, sem_out = refs[1 + parts * earlier + extras :]
    spans = spans_of(sums.shape[0], parts)

    def save(g):
        span = pl.ds(*spans[g])
        return pltpu.make_async_copy(
            out.at[span], potential.at[span, pl.ds(first * depth, width * depth)], sem_out.at[g]
        )

    for g, (start, length) in enumerate(spans):
        below = offsets[g * earlier : (g + 1) * earlier]

        def walk(y, carry):
            for x in range(width):
                row = pl.ds(x, depth, stride=0)
                total = below[0][y - start, row, :]
                for offset in below[1:]:
                    total = total + offset[y - start, row, :]
                span = pl.ds(x * depth, depth)
                out[y, span, :] = sums[y, span, :] + total
            return carry

        lax.fori_loop(start, start + length, walk, 0)
        save(g).start()
    for g in range(parts):
        save(g).wait()


def ring(axis):
    count = lax.axis_size(axis)
    forward = [(i, (i + 1) % count) for i in range(count)]
    return forward, [(target, origin) for origin, target in forward]


def on_device(tracer, conductance, source):
    shape = tracer.shape
    planes, columns, depth, members = shape
    pieces = pieces_of(columns)
    last_piece = len(pieces) - 1
    flat = (planes, columns * depth, members)
    tracer, conductance, source = (v.reshape(flat) for v in (tracer, conductance, source))
    count, _ = groups_of(planes)

    def far(*dims):
        return pltpu.HBM(dims, jnp.float32)

    def near(*dims):
        return pltpu.VMEM(dims, jnp.float32)

    def call(kernel, operands, specs, outs, out_specs, scratch=(), aliases=None):
        operands = [
            pltpu.with_memory_space_constraint(v, pltpu.VMEM if spec is VMEM else pltpu.HBM)
            for v, spec in zip(operands, specs)
        ]
        return pl.pallas_call(
            kernel,
            out_shape=outs,
            in_specs=specs,
            out_specs=out_specs,
            input_output_aliases=aliases or {},
            scratch_shapes=list(scratch),
            compiler_params=pltpu.CompilerParams(vmem_limit_bytes=VMEM_LIMIT),
        )(*operands)

    def ends(k):
        return int(k == 0), int(k == last_piece)

    def block(k):
        return near(planes, pieces[k][1] * depth, members)

    def outer_arrays(k):
        width = pieces[k][1]
        return [
            near(planes, width, members),
            near(planes, width, members),
            near(2, width * depth, members),
        ] + [near(planes, depth, members)] * sum(ends(k))

    def prepare(k, token):
        plan = (*pieces[k], depth, *ends(k), len(token))

        def kernel(*refs):
            prepare_kernel(plan, *refs)

        outs = [block(k)] + outer_arrays(k)
        return call(
            kernel,
            [tracer] + token,
            [HBM] + [VMEM] * len(token),
            outs,
            [VMEM] * len(outs),
            [pltpu.SemaphoreType.DMA((count,))],
        )

    def advance(k, step, where, operands, whole, token):
        first, width = pieces[k]
        load_rest, last = step == 0, step == STEPS - 1
        rest = HBM if load_rest else VMEM
        specs = [VMEM] * 7 + [rest] * 2 + [VMEM] * len(token)
        operands = operands + token
        aliases = {}
        if last and k > 0:
            aliases = {len(operands): 0}
            operands = operands + [whole]
            specs = specs + [HBM]
        parts = parts_of(k)
        plan = (width, depth, first, where, *ends(k), load_rest, last, parts, scale, len(operands) - 9)

        def kernel(*refs):
            step_kernel(plan, *refs)

        if last:
            outs = [far(*flat), block(k)]
            outs += [near(length, width, members) for _, length in spans_of(planes, parts)]
            out_specs = [HBM] + [VMEM] * (1 + parts)
            scratch = [
                pltpu.VMEM((planes, width * depth, members), jnp.float32),
                pltpu.SemaphoreType.DMA((parts,)),
            ]
        else:
            outs = [block(k)] + outer_arrays(k) + [block(k)] * (2 * load_rest)
            out_specs = [VMEM] * len(outs)
            scratch = [pltpu.SemaphoreType.DMA((2, count))] * load_rest
        return call(kernel, operands, specs, outs, out_specs, scratch, aliases)

    def finish(k, sums, offsets, whole):
        first, width = pieces[k]
        parts, earlier = len(offsets), len(offsets[0])
        operands = [sums] + [v for part in offsets for v in part]
        specs = [VMEM] * len(operands)
        aliases = {}
        if k > 0:
            aliases = {len(operands): 0}
            operands = operands + [whole]
            specs = specs + [HBM]
        extras = len(operands) - 1 - parts * earlier
        plan = (width, depth, first, parts, earlier, extras)

        def kernel(*refs):
            potential_kernel(plan, *refs)

        scratch = [
            pltpu.VMEM((planes, width * depth, members), jnp.float32),
            pltpu.SemaphoreType.DMA((parts,)),
        ]
        return call(kernel, operands, specs, [far(*flat)], [HBM], scratch, aliases)[0]

    blocks = lax.axis_size("pz")
    cells_along = depth * blocks
    exact = cells_along & (cells_along - 1) == 0
    scale = (1.0 / cells_along, True) if exact else (float(cells_along), False)
    z_up, z_down = ring("pz")
    y_up, y_down = ring("py")
    x_up, x_down = ring("px")

    def exchange(k, outer, sides):
        bottom, top, rows = outer[:3]
        edges = list(outer[3:])
        from_below = lax.ppermute(top, "pz", z_up)
        from_above = lax.ppermute(bottom, "pz", z_down)
        if len(y_up) <= 2:
            rows = lax.ppermute(rows, "py", y_up)
            lower_y, upper_y = (rows, 0), (rows, 1)
        else:
            lower_y = (lax.ppermute(rows[0:1], "py", y_up), 0)
            upper_y = (lax.ppermute(rows[1:2], "py", y_down), 0)
        lead, trail = ends(k)
        if lead:
            sides["right"] = lax.ppermute(edges.pop(0), "px", x_down)
        if trail:
            sides["left"] = lax.ppermute(edges.pop(0), "px", x_up)
        return lower_y, upper_y, from_below, from_above

    fields, rest, halos, sides, token = [], [], [], {}, []
    for k in range(len(pieces)):
        field, *outer = prepare(k, token)
        token = [outer[0]]
        fields.append(field)
        rest.append((conductance, source))
        halos.append(exchange(k, outer, sides))
    token = []
    end, totals = None, []
    for step in range(STEPS):
        next_fields, next_halos, next_sides = [], [], {}
        for k, (first, width) in enumerate(pieces):
            lower_y, upper_y, from_below, from_above = halos[k]
            left = (fields[k - 1], pieces[k - 1][1] - 1) if k > 0 else (sides["left"], 0)
            right = (fields[k + 1], 0) if k < last_piece else (sides["right"], 0)
            where = (left[1], right[1], lower_y[1], upper_y[1])
            operands = [fields[k], left[0], right[0], lower_y[0], upper_y[0]]
            operands += [from_below, from_above, *rest[k]]
            results = list(advance(k, step, where, operands, end, token))
            if step == STEPS - 1:
                end, field, *total = results
                token = []
                next_fields.append(field)
                totals.append(total)
                continue
            if step == 0:
                rest[k] = tuple(results[-2:])
                results = results[:-2]
            token = [results[1]]
            next_fields.append(results[0])
            next_halos.append(exchange(k, results[1:], next_sides))
        fields, halos, sides = next_fields, next_halos, next_sides

    potential = None
    for k in range(len(pieces)):
        offsets = []
        for carried in totals[k]:
            offsets.append([])
            for hop in range(blocks - 1):
                arrived = lax.ppermute(carried, "pz", [(hop, hop + 1)])
                offsets[-1].append(arrived)
                if hop < blocks - 2:
                    carried = carried + arrived
        potential = finish(k, fields[k], offsets, potential)
    return (potential.reshape(shape), end.reshape(shape))


def solution(mesh):
    placed = P("py", "px", "pz", None)

    return jax.shard_map(
        on_device,
        mesh=mesh,
        in_specs=(placed, placed, placed),
        out_specs=(placed, placed),
        check_vma=False,
    )
```
